32 devices in a mesh: blk: 8 (over z, x), rows: 4 (over y, core).
Axes of the slice: x: 2, y: 2, z: 4, core: 2. Of those that a mesh axis runs over, the one named last changes fastest.
Arguments:
- columns: float32 [512, 16384], P('blk', 'rows'), may hold values from -100 to 100
- plan: int32 [3, 16], replicated, may hold values from 0 to 15, as said below
Outputs:
- swept: float32 [512, 16384], P('blk', 'rows')
- off_ratio: float32 [3], replicated
The draws below stay inside these ranges and needn't reach their ends.
Inputs may be any that keep to these rules, and one draw needn't show every extreme that they name: `plan`: row s is a permutation of the 16 positions (position k is slot k % 2 of blk index k // 2). In each row there are a slot t and a number m of 1 to 7 such that the block in slot t of every blk index i goes to slot t of blk index (i + m) modulo 16 / 2, and every other block stays where it is.
All inputs are finite; a program needn't handle non-finite values. Where the reference program divides by a largest or mean magnitude, that divisor is 1e-20 or more.
Results may differ from the reference program's by a relative error of at most 0.00011.
Values sent between devices are 32-bit elements; how exact they have to be, the bound alone decides.
A program may use at most 64 MiB of HBM per device.

```python
import math
import jax
import jax.numpy as jnp
from jax import lax

BW = 32
STEPS = 3
EIG_ITERS = 3
NS_ITERS = 8
BLOCKS = 16
NCOL = 512
M = 16384


def draw_columns(key, part):
    keys = jax.random.split(jax.random.fold_in(key, 11), 2)
    position = jnp.arange(NCOL, dtype=jnp.float32) / NCOL
    scales = jnp.exp(jax.random.uniform(keys[0], (NCOL,), jnp.float32, 0.0, math.log(6.0)))
    entries = jax.random.normal(keys[1], (NCOL, M), jnp.float32)
    trend = 1.0 + 0.8 * position
    values = entries * (scales * trend)[:, None]
    return jnp.clip(values, -100.0, 100.0).astype(jnp.float32)


def draw_plan(key, part):
    keys = jax.random.split(jax.random.fold_in(key, 23), 2)
    half = BLOCKS // 2
    partner_steps = jax.random.randint(keys[0], (STEPS,), 1, half)
    leaving_slots = jax.random.randint(keys[1], (STEPS,), 0, 2)
    position = jnp.arange(BLOCKS, dtype=jnp.int32)
    device_index = position // 2
    slot_index = position % 2
    moved = (device_index[None, :] + partner_steps[:, None]) % half * 2 + slot_index[None, :]
    table = jnp.where(slot_index[None, :] == leaving_slots[:, None], moved, position[None, :])
    return table.astype(jnp.int32)


def setup_inputs(seed: int = 0) -> dict:
    key_of = jax.random.split(jax.random.key(seed), 3)
    return {
        "columns": draw_columns(jax.random.fold_in(key_of[2], 71), 0),
        "plan": draw_plan(jax.random.fold_in(key_of[2], 71), 0),
    }


PRECISE = lax.Precision.HIGHEST

def matmul(left, right):
    return jnp.matmul(left, right, precision=PRECISE, preferred_element_type=jnp.float32)

def flipped(matrix):
    return jnp.swapaxes(matrix, -1, -2)

def orthonormal(matrix):
    lengths = jnp.sqrt(lax.optimization_barrier(jnp.sum(matrix * matrix, axis=-2, keepdims=True)))
    normed = matrix / lengths
    inner = matmul(flipped(normed), normed)
    bound = lax.optimization_barrier(jnp.max(lax.optimization_barrier(jnp.sum(jnp.abs(inner), axis=-1)), axis=-1))
    normed = normed / jnp.sqrt(bound)[..., None, None]
    for turn_index in range(NS_ITERS):
        normed = 1.5 * normed - 0.5 * matmul(normed, matmul(flipped(normed), normed))
    return normed

def pair_rotation(gram_sum):
    rotation = jnp.broadcast_to(jnp.eye(gram_sum.shape[-1], dtype=gram_sum.dtype), gram_sum.shape)
    for turn_index in range(EIG_ITERS):
        rotation = orthonormal(matmul(gram_sum, rotation))
    return rotation

def reference(columns, plan):
    current = columns
    eye_mask = jnp.eye(2 * BW, dtype=bool)
    ratios = []
    for step_index in range(STEPS):
        pairs = current.reshape(BLOCKS // 2, 2 * BW, M)
        gram_sum = matmul(pairs, flipped(pairs))
        off_part = jnp.where(eye_mask, 0.0, gram_sum)
        diag_part = jnp.where(eye_mask, gram_sum, 0.0)
        off_total = jnp.sum(off_part * off_part)
        diag_total = jnp.sum(diag_part * diag_part)
        ratios.append(jnp.sqrt(off_total) / jnp.sqrt(diag_total))
        rotation = pair_rotation(gram_sum)
        rotated = matmul(flipped(rotation), pairs)
        blocks = rotated.reshape(BLOCKS, BW, M)
        placed = jnp.zeros_like(blocks).at[plan[step_index]].set(blocks)
        current = placed.reshape(NCOL, M)
    return (current, jnp.stack(ratios))
```

```python
from functools import partial

import jax
import jax.numpy as jnp
from jax import lax
from jax.experimental import pallas as pl
from jax.experimental.pallas import tpu as pltpu
from jax.sharding import PartitionSpec as P

EIG_ITERS = 3
NS_ITERS = 8
MESH = pl.DeviceIdType.MESH


def split(value):
    high = value.astype(jnp.bfloat16)
    low = (value - high.astype(jnp.float32)).astype(jnp.bfloat16)
    return high, low


def left_of(value):
    high = value.astype(jnp.bfloat16).astype(jnp.float32)
    low = value - high
    lane = lax.broadcasted_iota(jnp.int32, value.shape, 1)
    mixed = jnp.where(lane < value.shape[1] // 2, high, low).astype(jnp.bfloat16)
    return jnp.concatenate([mixed, mixed], axis=1)


def right_of(value):
    high, low = split(value)
    return jnp.concatenate([high, high, low, low], axis=0)


def dot(left, right):
    return jnp.dot(left, right, preferred_element_type=jnp.float32)


def orthonormal(z, zt):
    y = z / jnp.sqrt(jnp.sum(z * z, axis=0, keepdims=True))
    t = zt / jnp.sqrt(0.5 * jnp.sum(zt * zt, axis=1, keepdims=True))
    inner = dot(left_of(t), right_of(y))
    bound = jnp.max(jnp.sum(jnp.abs(inner), axis=0, keepdims=True), axis=1, keepdims=True)
    root = jnp.sqrt(bound)
    y = y / root
    t = t / root

    def turn(_, carry):
        y, t = carry
        inner = dot(left_of(t), right_of(y))
        y_next = 1.5 * y - 0.5 * dot(left_of(y), right_of(inner))
        t_next = 1.5 * t - 0.5 * dot(left_of(inner), right_of(t))
        return y_next, t_next

    return lax.fori_loop(0, NS_ITERS, turn, (y, t))


def step_kernel(last, flag_ref, stay_ref, move_ref, seen_ref, out_stay_ref, out_move_ref, stat_ref,
                grams, sums, send_sem, recv_sem, stat_send, stat_recv):
    half = stay_ref.shape[0]
    width = 2 * half
    share = stay_ref.shape[1]
    count = lax.axis_size("rows")
    others = lax.axis_size("blk")
    me = lax.axis_index("rows")
    mine = lax.axis_index("blk")

    barrier = pltpu.get_barrier_semaphore()
    for distance in range(1, count):
        peer = lax.rem(me + distance, count)
        pl.semaphore_signal(barrier, inc=1, device_id={"rows": peer}, device_id_type=MESH)
    greeted = count - 1
    if last:
        for distance in range(1, others):
            peer = lax.rem(mine + distance, others)
            pl.semaphore_signal(barrier, inc=1, device_id={"blk": peer}, device_id_type=MESH)
        greeted += others - 1

    stay_high, stay_low = split(stay_ref[...])
    move_high, move_low = split(move_ref[...])
    stacked = jnp.concatenate([stay_high, move_high, stay_low, move_low], axis=0)
    products = lax.dot_general(stacked, stacked, (((1,), (1,)), ((), ())),
                               preferred_element_type=jnp.float32)
    folded = products + pltpu.roll(products, width, 1)
    gram = folded[:width] + folded[width:]
    lane = lax.broadcasted_iota(jnp.int32, (half, 2 * width), 1)
    grams[me] = jnp.where(lane < width, gram[:half], gram[half:])

    pl.semaphore_wait(barrier, greeted)
    copies = []
    for distance in range(1, count):
        peer = lax.rem(me + distance, count)
        copy = pltpu.make_async_remote_copy(
            src_ref=grams.at[me], dst_ref=grams.at[me],
            send_sem=send_sem.at[distance - 1], recv_sem=recv_sem.at[distance - 1],
            device_id={"rows": peer}, device_id_type=MESH)
        copy.start()
        copies.append(copy)
    for copy in copies:
        copy.wait()
    packed = grams[0]
    for index in range(1, count):
        packed = packed + grams[index]
    turned = pltpu.roll(packed, width, 1)
    gram = jnp.concatenate([jnp.where(lane < width, packed, turned),
                            jnp.where(lane < width, turned, packed)], axis=0)

    row = lax.broadcasted_iota(jnp.int32, gram.shape, 0)
    column = lax.broadcasted_iota(jnp.int32, gram.shape, 1)
    square = gram * gram
    diag_part = jnp.where(row == column, square, 0.0)
    off_part = jnp.where((row == column) | (column >= width), 0.0, square)
    off_total = jnp.sum(jnp.sum(off_part, axis=0, keepdims=True), axis=1, keepdims=True)
    diag_total = jnp.sum(jnp.sum(diag_part, axis=0, keepdims=True), axis=1, keepdims=True)
    line = lax.broadcasted_iota(jnp.int32, seen_ref.shape, 0)
    at_lane = lax.broadcasted_iota(jnp.int32, seen_ref.shape, 1)
    base = flag_ref[1]
    fresh = jnp.where(line == 0, off_total, diag_total)
    totals = jnp.where((at_lane == base) & (line < 2), fresh, seen_ref[...])
    stat_copies = []
    if last:
        sums[mine] = totals
        for distance in range(1, others):
            peer = lax.rem(mine + distance, others)
            copy = pltpu.make_async_remote_copy(
                src_ref=sums.at[mine], dst_ref=sums.at[mine],
                send_sem=stat_send.at[distance - 1], recv_sem=stat_recv.at[distance - 1],
                device_id={"blk": peer}, device_id_type=MESH)
            copy.start()
            stat_copies.append(copy)
    else:
        stat_ref[...] = totals

    q, t = orthonormal(gram, gram)
    gram_left, gram_right = left_of(gram), right_of(gram)
    for _ in range(1, EIG_ITERS):
        z = dot(gram_left, right_of(q))
        zt = dot(left_of(t), gram_right)
        q, t = orthonormal(z, zt)

    leaving_last = flag_ref[0] == 1
    t_stay = jnp.where(leaving_last, t[:half], t[half:])
    t_move = jnp.where(leaving_last, t[half:], t[:half])
    left = left_of(jnp.concatenate([t_stay, t_move], axis=0))
    chunk = min(512, share)
    for start in range(0, share, chunk):
        where = pl.ds(start, chunk)
        right = right_of(jnp.concatenate([stay_ref[:, where], move_ref[:, where]], axis=0))
        rotated = dot(left, right)
        out_stay_ref[:, where] = rotated[:half]
        out_move_ref[:, where] = rotated[half:]

    if last:
        for copy in stat_copies:
            copy.wait()
        total = sums[0]
        for index in range(1, others):
            total = total + sums[index]
        ratio = jnp.sqrt(total[0:1]) / jnp.sqrt(total[1:2])
        stat_ref[...] = jnp.broadcast_to(ratio, stat_ref.shape)


def step_call(last, flags, stay, move, seen):
    half, share = stay.shape
    count = lax.axis_size("rows")
    others = lax.axis_size("blk")
    vmem = pl.BlockSpec(memory_space=pltpu.VMEM)
    return pl.pallas_call(
        partial(step_kernel, last),
        out_shape=(
            jax.ShapeDtypeStruct((half, share), jnp.float32),
            jax.ShapeDtypeStruct((half, share), jnp.float32),
            jax.ShapeDtypeStruct(seen.shape, jnp.float32),
        ),
        in_specs=[pl.BlockSpec(memory_space=pltpu.SMEM), vmem, vmem, vmem],
        out_specs=(vmem, vmem, vmem),
        scratch_shapes=[
            pltpu.VMEM((count, half, 4 * half), jnp.float32),
            pltpu.VMEM((others if last else 1,) + seen.shape, jnp.float32),
            pltpu.SemaphoreType.DMA((max(count - 1, 1),)),
            pltpu.SemaphoreType.DMA((max(count - 1, 1),)),
            pltpu.SemaphoreType.DMA((max(others - 1, 1),)),
            pltpu.SemaphoreType.DMA((max(others - 1, 1),)),
        ],
        compiler_params=pltpu.CompilerParams(
            collective_id=1 if last else 0, has_side_effects=True),
        name="last_step" if last else "step",
    )(flags, stay, move, seen)


def move_by(values, distance):
    count = lax.axis_size("blk")
    pairs = [(source, (source + distance) % count) for source in range(count)]
    return lax.ppermute(values, "blk", pairs)


def local(columns, plan):
    steps = plan.shape[0]
    half = columns.shape[0] // 2
    count = lax.axis_size("blk")
    branches = [partial(move_by, distance=distance) for distance in range(1, count)]
    stay, move = columns[:half], columns[half:]
    second_slot = jnp.int32(1)
    seen = jnp.zeros((8, 128), jnp.float32)
    for step_index in range(steps):
        first_dest = plan[step_index, 0]
        second_dest = plan[step_index, 1]
        distance = jnp.maximum(first_dest // 2, second_dest // 2)
        leaving_slot = (second_dest != 1).astype(jnp.int32)
        leaving_last = (leaving_slot == second_slot).astype(jnp.int32)
        flags = jnp.stack([leaving_last, jnp.int32(step_index)])
        stay, move, seen = step_call(step_index == steps - 1, flags, stay, move, seen)
        move = lax.switch(distance - 1, branches, move)
        second_slot = leaving_slot
    current = jnp.where(
        second_slot == 1,
        jnp.concatenate([stay, move], axis=0),
        jnp.concatenate([move, stay], axis=0),
    )
    return current, seen[0, :steps]


def solution(mesh):
    return jax.shard_map(
        local,
        mesh=mesh,
        in_specs=(P("blk", "rows"), P()),
        out_specs=(P("blk", "rows"), P()),
        check_vma=False,
    )
```

```python
from functools import partial

import jax
import jax.numpy as jnp
from jax import lax
from jax.experimental import pallas as pl
from jax.experimental.pallas import tpu as pltpu
from jax.sharding import PartitionSpec as P

EIG_ITERS = 3
NS_ITERS = 8
CHUNKS = 3
MESH = pl.DeviceIdType.MESH


def split(value):
    high = value.astype(jnp.bfloat16)
    low = (value - high.astype(jnp.float32)).astype(jnp.bfloat16)
    return high, low


def left_of(value):
    high = value.astype(jnp.bfloat16).astype(jnp.float32)
    low = value - high
    lane = lax.broadcasted_iota(jnp.int32, value.shape, 1)
    mixed = jnp.where(lane < value.shape[1] // 2, high, low).astype(jnp.bfloat16)
    return jnp.concatenate([mixed, mixed], axis=1)


def right_of(value):
    high, low = split(value)
    return jnp.concatenate([high, high, low, low], axis=0)


def dot(left, right):
    return jnp.dot(left, right, preferred_element_type=jnp.float32)


def orthonormal(z, zt):
    y = z / jnp.sqrt(jnp.sum(z * z, axis=0, keepdims=True))
    t = zt / jnp.sqrt(0.5 * jnp.sum(zt * zt, axis=1, keepdims=True))
    inner = dot(left_of(t), right_of(y))
    bound = jnp.max(jnp.sum(jnp.abs(inner), axis=0, keepdims=True), axis=1, keepdims=True)
    root = jnp.sqrt(bound)
    y = y / root
    t = t / root

    def turn(_, carry):
        y, t = carry
        inner = dot(left_of(t), right_of(y))
        y_next = 1.5 * y - 0.5 * dot(left_of(y), right_of(inner))
        t_next = 1.5 * t - 0.5 * dot(left_of(inner), right_of(t))
        return y_next, t_next

    return lax.fori_loop(0, NS_ITERS, turn, (y, t))


def early_share(share, distance, count):
    part = 1 if 4 * distance > count and 4 * distance < 3 * count else 2
    return max(share // 1024 * 256 * part - (256 if part == 2 else 0), 0)


def step_kernel(step, last, distance, plan_ref, current_ref, seen_ref, out_ref, stat_ref,
                grams, sums, early, turning, turning_in, leaving,
                send_sem, recv_sem, stat_send, stat_recv, move_send, move_recv):
    width, share = current_ref.shape
    half = width // 2
    count = lax.axis_size("rows")
    others = lax.axis_size("blk")
    me = lax.axis_index("rows")
    mine = lax.axis_index("blk")
    target = lax.rem(mine + distance, others)
    source = lax.rem(mine + others - distance, others)
    early_lanes = early.shape[1]
    chunk = leaving.shape[1] // CHUNKS

    barrier = pltpu.get_barrier_semaphore()
    for offset in range(1, count):
        peer = lax.rem(me + offset, count)
        pl.semaphore_signal(barrier, inc=1, device_id={"rows": peer}, device_id_type=MESH)
    greeted = count - 1
    if last:
        for offset in range(1, others):
            peer = lax.rem(mine + offset, others)
            pl.semaphore_signal(barrier, inc=1, device_id={"blk": peer}, device_id_type=MESH)
        greeted += others - 1
    else:
        for peer in (target, source):
            pl.semaphore_signal(barrier, inc=1, device_id={"blk": peer}, device_id_type=MESH)
        greeted += 2
    pl.semaphore_wait(barrier, greeted)

    def forward(src, dst, index):
        copy = pltpu.make_async_remote_copy(
            src_ref=src, dst_ref=dst,
            send_sem=move_send.at[index], recv_sem=move_recv.at[index],
            device_id={"blk": target}, device_id_type=MESH)
        copy.start()
        return copy

    early_copy = forward(current_ref.at[:, pl.ds(0, early_lanes)], early, 0)

    high, low = split(current_ref[...])
    stacked = jnp.concatenate([high, low], axis=0)
    products = lax.dot_general(stacked, stacked, (((1,), (1,)), ((), ())),
                               preferred_element_type=jnp.float32)
    folded = products + pltpu.roll(products, width, 1)
    gram = folded[:width] + folded[width:]
    lane = lax.broadcasted_iota(jnp.int32, (half, 2 * width), 1)
    grams[me] = jnp.where(lane < width, gram[:half], gram[half:])

    copies = []
    for offset in range(1, count):
        peer = lax.rem(me + offset, count)
        copy = pltpu.make_async_remote_copy(
            src_ref=grams.at[me], dst_ref=grams.at[me],
            send_sem=send_sem.at[offset - 1], recv_sem=recv_sem.at[offset - 1],
            device_id={"rows": peer}, device_id_type=MESH)
        copy.start()
        copies.append(copy)
    for copy in copies:
        copy.wait()
    packed = grams[0]
    for index in range(1, count):
        packed = packed + grams[index]
    turned = pltpu.roll(packed, width, 1)
    gram = jnp.concatenate([jnp.where(lane < width, packed, turned),
                            jnp.where(lane < width, turned, packed)], axis=0)

    row = lax.broadcasted_iota(jnp.int32, gram.shape, 0)
    column = lax.broadcasted_iota(jnp.int32, gram.shape, 1)
    square = gram * gram
    diag_part = jnp.where(row == column, square, 0.0)
    off_part = jnp.where((row == column) | (column >= width), 0.0, square)
    off_total = jnp.sum(jnp.sum(off_part, axis=0, keepdims=True), axis=1, keepdims=True)
    diag_total = jnp.sum(jnp.sum(diag_part, axis=0, keepdims=True), axis=1, keepdims=True)
    line = lax.broadcasted_iota(jnp.int32, seen_ref.shape, 0)
    at_lane = lax.broadcasted_iota(jnp.int32, seen_ref.shape, 1)
    fresh = jnp.where(line == 0, off_total, diag_total)
    before = jnp.zeros(seen_ref.shape, jnp.float32) if step == 0 else seen_ref[...]
    totals = jnp.where((at_lane == step) & (line < 2), fresh, before)
    stat_copies = []
    if last:
        sums[mine] = totals
        for offset in range(1, others):
            peer = lax.rem(mine + offset, others)
            copy = pltpu.make_async_remote_copy(
                src_ref=sums.at[mine], dst_ref=sums.at[mine],
                send_sem=stat_send.at[offset - 1], recv_sem=stat_recv.at[offset - 1],
                device_id={"blk": peer}, device_id_type=MESH)
            copy.start()
            stat_copies.append(copy)
    else:
        stat_ref[...] = totals

    q, t = orthonormal(gram, gram)
    gram_left, gram_right = left_of(gram), right_of(gram)
    for _ in range(1, EIG_ITERS):
        z = dot(gram_left, right_of(q))
        zt = dot(left_of(t), gram_right)
        q, t = orthonormal(z, zt)

    leaving_slot = jnp.where(plan_ref[step, 1] != 1, 1, 0)
    second_slot = 1 if step == 0 else jnp.where(plan_ref[step - 1, 1] != 1, 1, 0)
    leaving_last = leaving_slot == second_slot
    t_stay = jnp.where(leaving_last, t[:half], t[half:])
    t_move = jnp.where(leaving_last, t[half:], t[:half])
    turning[...] = t_move
    turn_copy = forward(turning, turning_in, 1)
    left = left_of(jnp.concatenate([t_stay, t_move], axis=0))
    moves = []
    for index in range(CHUNKS):
        where = pl.ds(early_lanes + index * chunk, chunk)
        there = pl.ds(index * chunk, chunk)
        rotated = dot(left, right_of(current_ref[:, where]))
        leaving[:, there] = rotated[half:]
        moves.append(forward(leaving.at[:, there], out_ref.at[pl.ds(half, half), where], 2 + index))
        out_ref[pl.ds(0, half), where] = rotated[:half]
    left_stay = left_of(t_stay)
    piece = 256
    for start in range(0, early_lanes, piece):
        where = pl.ds(start, piece)
        out_ref[pl.ds(0, half), where] = dot(left_stay, right_of(current_ref[:, where]))

    early_copy.wait()
    turn_copy.wait()
    left_move = left_of(turning_in[...])
    for start in range(0, early_lanes, piece):
        where = pl.ds(start, piece)
        out_ref[pl.ds(half, half), where] = dot(left_move, right_of(early[:, where]))

    if last:
        for copy in stat_copies:
            copy.wait()
        total = sums[0]
        for index in range(1, others):
            total = total + sums[index]
        ratio = jnp.sqrt(total[0:1]) / jnp.sqrt(total[1:2])
        stat_ref[...] = jnp.broadcast_to(ratio, stat_ref.shape)
    for copy in moves:
        copy.wait()


def step_call(plan, current, seen, step, last, distance):
    width, share = current.shape
    half = width // 2
    count = lax.axis_size("rows")
    others = lax.axis_size("blk")
    early_lanes = early_share(share, distance, others)
    vmem = pl.BlockSpec(memory_space=pltpu.VMEM)
    return pl.pallas_call(
        partial(step_kernel, step, last, distance),
        out_shape=(
            jax.ShapeDtypeStruct(current.shape, jnp.float32),
            jax.ShapeDtypeStruct(seen.shape, jnp.float32),
        ),
        in_specs=[pl.BlockSpec(memory_space=pltpu.SMEM), vmem, vmem],
        out_specs=(vmem, vmem),
        scratch_shapes=[
            pltpu.VMEM((count, half, 2 * width), jnp.float32),
            pltpu.VMEM((others if last else 1,) + seen.shape, jnp.float32),
            pltpu.VMEM((width, early_lanes), jnp.float32),
            pltpu.VMEM((half, 2 * width), jnp.float32),
            pltpu.VMEM((half, 2 * width), jnp.float32),
            pltpu.VMEM((half, share - early_lanes), jnp.float32),
            pltpu.SemaphoreType.DMA((max(count - 1, 1),)),
            pltpu.SemaphoreType.DMA((max(count - 1, 1),)),
            pltpu.SemaphoreType.DMA((max(others - 1, 1),)),
            pltpu.SemaphoreType.DMA((max(others - 1, 1),)),
            pltpu.SemaphoreType.DMA((2 + CHUNKS,)),
            pltpu.SemaphoreType.DMA((2 + CHUNKS,)),
        ],
        compiler_params=pltpu.CompilerParams(
            collective_id=step * (others - 1) + distance - 1, has_side_effects=True),
        name=f"step{step}_by{distance}",
    )(plan, current, seen)


def place_kernel(plan_ref, current_ref, stat_ref, out_ref, ratio_ref, sems):
    width = current_ref.shape[0]
    half = width // 2
    steps = ratio_ref.shape[0]
    leaving = jnp.where(plan_ref[steps - 1, 1] != 1, 1, 0)
    copies = []
    for index, slot in enumerate((1 - leaving, leaving)):
        copy = pltpu.make_async_copy(
            current_ref.at[pl.ds(index * half, half)],
            out_ref.at[pl.ds(pl.multiple_of(slot * half, half), half)], sems.at[index])
        copy.start()
        copies.append(copy)
    lane = lax.broadcasted_iota(jnp.int32, stat_ref.shape, 1)
    line = lax.broadcasted_iota(jnp.int32, stat_ref.shape, 0)
    values = stat_ref[...]
    for index in range(steps):
        ratio_ref[index] = jnp.sum(jnp.where((lane == index) & (line == 0), values, 0.0))
    for copy in copies:
        copy.wait()


def local(columns, plan):
    steps = plan.shape[0]
    count = lax.axis_size("blk")
    current = columns
    seen = jnp.zeros((8, 128), jnp.float32)
    for step in range(steps):
        first_dest = plan[step, 0]
        second_dest = plan[step, 1]
        distance = jnp.maximum(first_dest // 2, second_dest // 2)
        branches = [partial(step_call, step=step, last=step == steps - 1, distance=d) for d in range(1, count)]
        current, seen = lax.switch(distance - 1, branches, plan, current, seen)
    vmem = pl.BlockSpec(memory_space=pltpu.VMEM)
    return pl.pallas_call(
        place_kernel,
        out_shape=(
            jax.ShapeDtypeStruct(columns.shape, jnp.float32),
            jax.ShapeDtypeStruct((steps,), jnp.float32),
        ),
        in_specs=[pl.BlockSpec(memory_space=pltpu.SMEM), vmem, vmem],
        out_specs=(pl.BlockSpec(memory_space=pl.ANY), pl.BlockSpec(memory_space=pltpu.SMEM)),
        scratch_shapes=[pltpu.SemaphoreType.DMA((2,))],
        name="place",
    )(plan, current, seen)


def solution(mesh):
    return jax.shard_map(
        local,
        mesh=mesh,
        in_specs=(P("blk", "rows"), P()),
        out_specs=(P("blk", "rows"), P()),
        check_vma=False,
    )
```

```python
from functools import partial

import jax
import jax.numpy as jnp
from jax import lax
from jax.experimental import pallas as pl
from jax.experimental.pallas import tpu as pltpu
from jax.sharding import PartitionSpec as P

EIG_ITERS = 3
NS_ITERS = 8
CHUNKS = 2
NEAR_PART = 9
MESH = pl.DeviceIdType.MESH


def split(value):
    high = value.astype(jnp.bfloat16)
    low = (value - high.astype(jnp.float32)).astype(jnp.bfloat16)
    return high, low


def left_of(value):
    high = value.astype(jnp.bfloat16).astype(jnp.float32)
    low = value - high
    lane = lax.broadcasted_iota(jnp.int32, value.shape, 1)
    mixed = jnp.where(lane < value.shape[1] // 2, high, low).astype(jnp.bfloat16)
    return jnp.concatenate([mixed, mixed], axis=1)


def right_of(value):
    high, low = split(value)
    return jnp.concatenate([high, high, low, low], axis=0)


def dot(left, right):
    return jnp.dot(left, right, preferred_element_type=jnp.float32)


def orthonormal(z, zt):
    y = z / jnp.sqrt(jnp.sum(z * z, axis=0, keepdims=True))
    t = zt / jnp.sqrt(0.5 * jnp.sum(zt * zt, axis=1, keepdims=True))
    inner = dot(left_of(t), right_of(y))
    bound = jnp.max(jnp.sum(jnp.abs(inner), axis=0, keepdims=True), axis=1, keepdims=True)
    root = jnp.sqrt(bound)
    y = y / root
    t = t / root

    def turn(_, carry):
        y, t = carry
        inner = dot(left_of(t), right_of(y))
        y_next = 1.5 * y - 0.5 * dot(left_of(y), right_of(inner))
        t_next = 1.5 * t - 0.5 * dot(left_of(inner), right_of(t))
        return y_next, t_next

    return lax.fori_loop(0, NS_ITERS, turn, (y, t))


def early_share(share, distance, count):
    part = 4 if 4 * distance > count and 4 * distance < 3 * count else NEAR_PART
    return max(share * part // 16 // 256 * 256, 256)


def step_kernel(step, last, distance, plan_ref, current_ref, *refs):
    seen_ref = refs[0] if step else None
    (out_ref, stat_ref, grams, sums, early, turning, turning_in, leaving,
     send_sem, recv_sem, stat_send, stat_recv, move_send, move_recv) = refs[1 if step else 0:]
    width, share = current_ref.shape
    half = width // 2
    count = lax.axis_size("rows")
    others = lax.axis_size("blk")
    me = lax.axis_index("rows")
    mine = lax.axis_index("blk")
    target = lax.rem(mine + distance, others)
    source = lax.rem(mine + others - distance, others)
    early_lanes = early.shape[1]
    chunk = leaving.shape[1] // CHUNKS

    barrier = pltpu.get_barrier_semaphore()
    for offset in range(1, count):
        peer = lax.rem(me + offset, count)
        pl.semaphore_signal(barrier, inc=1, device_id={"rows": peer}, device_id_type=MESH)
    greeted = count - 1
    if last:
        for offset in range(1, others):
            peer = lax.rem(mine + offset, others)
            pl.semaphore_signal(barrier, inc=1, device_id={"blk": peer}, device_id_type=MESH)
        greeted += others - 1
    else:
        for peer in (target, source):
            pl.semaphore_signal(barrier, inc=1, device_id={"blk": peer}, device_id_type=MESH)
        greeted += 2
    def forward(src, dst, index):
        copy = pltpu.make_async_remote_copy(
            src_ref=src, dst_ref=dst,
            send_sem=move_send.at[index], recv_sem=move_recv.at[index],
            device_id={"blk": target}, device_id_type=MESH)
        copy.start()
        return copy

    high, low = split(current_ref[...])
    stacked = jnp.concatenate([high, low], axis=0)
    products = lax.dot_general(stacked, stacked, (((1,), (1,)), ((), ())),
                               preferred_element_type=jnp.float32)
    folded = products + pltpu.roll(products, width, 1)
    gram = folded[:width] + folded[width:]
    lane = lax.broadcasted_iota(jnp.int32, (half, 2 * width), 1)
    grams[me] = jnp.where(lane < width, gram[:half], gram[half:])

    pl.semaphore_wait(barrier, greeted)
    copies = []
    for offset in range(1, count):
        peer = lax.rem(me + offset, count)
        copy = pltpu.make_async_remote_copy(
            src_ref=grams.at[me], dst_ref=grams.at[me],
            send_sem=send_sem.at[offset - 1], recv_sem=recv_sem.at[offset - 1],
            device_id={"rows": peer}, device_id_type=MESH)
        copy.start()
        copies.append(copy)
    early_copy = forward(current_ref.at[:, pl.ds(0, early_lanes)], early, 0)
    for copy in copies:
        copy.wait()
    packed = grams[0]
    for index in range(1, count):
        packed = packed + grams[index]
    turned = pltpu.roll(packed, width, 1)
    gram = jnp.concatenate([jnp.where(lane < width, packed, turned),
                            jnp.where(lane < width, turned, packed)], axis=0)

    row = lax.broadcasted_iota(jnp.int32, gram.shape, 0)
    column = lax.broadcasted_iota(jnp.int32, gram.shape, 1)
    square = gram * gram
    diag_part = jnp.where(row == column, square, 0.0)
    off_part = jnp.where((row == column) | (column >= width), 0.0, square)
    off_total = jnp.sum(jnp.sum(off_part, axis=0, keepdims=True), axis=1, keepdims=True)
    diag_total = jnp.sum(jnp.sum(diag_part, axis=0, keepdims=True), axis=1, keepdims=True)
    line = lax.broadcasted_iota(jnp.int32, stat_ref.shape, 0)
    at_lane = lax.broadcasted_iota(jnp.int32, stat_ref.shape, 1)
    fresh = jnp.where(line == 0, off_total, diag_total)
    before = seen_ref[...] if step else jnp.zeros(stat_ref.shape, jnp.float32)
    totals = jnp.where((at_lane == step) & (line < 2), fresh, before)
    stat_copies = []
    if last:
        sums[mine] = totals
        for offset in range(1, others):
            peer = lax.rem(mine + offset, others)
            copy = pltpu.make_async_remote_copy(
                src_ref=sums.at[mine], dst_ref=sums.at[mine],
                send_sem=stat_send.at[offset - 1], recv_sem=stat_recv.at[offset - 1],
                device_id={"blk": peer}, device_id_type=MESH)
            copy.start()
            stat_copies.append(copy)
    else:
        stat_ref[...] = totals

    q, t = orthonormal(gram, gram)
    gram_left, gram_right = left_of(gram), right_of(gram)

    def again(_, carry):
        q, t = carry
        return orthonormal(dot(gram_left, right_of(q)), dot(left_of(t), gram_right))

    q, t = lax.fori_loop(1, EIG_ITERS, again, (q, t))

    leaving_slot = jnp.where(plan_ref[step, 1] != 1, 1, 0)
    second_slot = 1 if step == 0 else jnp.where(plan_ref[step - 1, 1] != 1, 1, 0)
    leaving_last = leaving_slot == second_slot
    t_stay = jnp.where(leaving_last, t[:half], t[half:])
    t_move = jnp.where(leaving_last, t[half:], t[:half])
    turning[...] = t_move
    turn_copy = forward(turning, turning_in, 1)
    left = left_of(jnp.concatenate([t_stay, t_move], axis=0))
    moves = []
    for index in range(CHUNKS):
        where = pl.ds(early_lanes + index * chunk, chunk)
        there = pl.ds(index * chunk, chunk)
        rotated = dot(left, right_of(current_ref[:, where]))
        leaving[:, there] = rotated[half:]
        moves.append(forward(leaving.at[:, there], out_ref.at[pl.ds(half, half), where], 2 + index))
        out_ref[pl.ds(0, half), where] = rotated[:half]
    left_stay = left_of(t_stay)
    piece = 256
    for start in range(0, early_lanes, piece):
        where = pl.ds(start, piece)
        out_ref[pl.ds(0, half), where] = dot(left_stay, right_of(current_ref[:, where]))

    early_copy.wait()
    turn_copy.wait()
    left_move = left_of(turning_in[...])
    for start in range(0, early_lanes, piece):
        where = pl.ds(start, piece)
        out_ref[pl.ds(half, half), where] = dot(left_move, right_of(early[:, where]))

    if last:
        for copy in stat_copies:
            copy.wait()
        total = sums[0]
        for index in range(1, others):
            total = total + sums[index]
        ratio = jnp.sqrt(total[0:1]) / jnp.sqrt(total[1:2])
        stat_ref[...] = jnp.broadcast_to(ratio, stat_ref.shape)
    for copy in moves:
        copy.wait()


def step_call(plan, current, *seen, step, last, distance):
    width, share = current.shape
    half = width // 2
    count = lax.axis_size("rows")
    others = lax.axis_size("blk")
    early_lanes = early_share(share, distance, others)
    vmem = pl.BlockSpec(memory_space=pltpu.VMEM)
    return pl.pallas_call(
        partial(step_kernel, step, last, distance),
        out_shape=(
            jax.ShapeDtypeStruct(current.shape, jnp.float32),
            jax.ShapeDtypeStruct((8, 128), jnp.float32),
        ),
        in_specs=[pl.BlockSpec(memory_space=pltpu.SMEM), vmem] + [vmem] * len(seen),
        out_specs=(vmem, vmem),
        scratch_shapes=[
            pltpu.VMEM((count, half, 2 * width), jnp.float32),
            pltpu.VMEM((others if last else 1, 8, 128), jnp.float32),
            pltpu.VMEM((width, early_lanes), jnp.float32),
            pltpu.VMEM((half, 2 * width), jnp.float32),
            pltpu.VMEM((half, 2 * width), jnp.float32),
            pltpu.VMEM((half, share - early_lanes), jnp.float32),
            pltpu.SemaphoreType.DMA((max(count - 1, 1),)),
            pltpu.SemaphoreType.DMA((max(count - 1, 1),)),
            pltpu.SemaphoreType.DMA((max(others - 1, 1),)),
            pltpu.SemaphoreType.DMA((max(others - 1, 1),)),
            pltpu.SemaphoreType.DMA((2 + CHUNKS,)),
            pltpu.SemaphoreType.DMA((2 + CHUNKS,)),
        ],
        compiler_params=pltpu.CompilerParams(
            collective_id=step * (others - 1) + distance - 1, has_side_effects=True),
        name=f"step{step}_by{distance}",
    )(plan, current, *seen)


def place_kernel(plan_ref, current_ref, stat_ref, out_ref, ratio_ref, sems):
    width = current_ref.shape[0]
    half = width // 2
    steps = ratio_ref.shape[0]
    leaving = jnp.where(plan_ref[steps - 1, 1] != 1, 1, 0)
    copies = []
    for index, slot in enumerate((1 - leaving, leaving)):
        copy = pltpu.make_async_copy(
            current_ref.at[pl.ds(index * half, half)],
            out_ref.at[pl.ds(pl.multiple_of(slot * half, half), half)], sems.at[index])
        copy.start()
        copies.append(copy)
    lane = lax.broadcasted_iota(jnp.int32, stat_ref.shape, 1)
    line = lax.broadcasted_iota(jnp.int32, stat_ref.shape, 0)
    values = stat_ref[...]
    for index in range(steps):
        ratio_ref[index] = jnp.sum(jnp.where((lane == index) & (line == 0), values, 0.0))
    for copy in copies:
        copy.wait()


def shift_kernel(plan_ref, *shift_refs):
    for step, shift_ref in enumerate(shift_refs):
        shift_ref[0] = jnp.maximum(plan_ref[step, 0] >> 1, plan_ref[step, 1] >> 1) - 1


def shift_call(plan):
    smem = pl.BlockSpec(memory_space=pltpu.SMEM)
    steps = plan.shape[0]
    return pl.pallas_call(
        shift_kernel,
        out_shape=tuple(jax.ShapeDtypeStruct((1,), jnp.int32) for _ in range(steps)),
        in_specs=[smem],
        out_specs=(smem,) * steps,
        name="shift",
    )(plan)


def local(columns, plan):
    steps = plan.shape[0]
    count = lax.axis_size("blk")
    current = columns
    seen = ()
    shifts = shift_call(plan)
    for step in range(steps):
        branches = [partial(step_call, step=step, last=step == steps - 1, distance=d) for d in range(1, count)]
        current, stat = lax.switch(shifts[step].reshape(()), branches, plan, current, *seen)
        seen = (stat,)
    vmem = pl.BlockSpec(memory_space=pltpu.VMEM)
    return pl.pallas_call(
        place_kernel,
        out_shape=(
            jax.ShapeDtypeStruct(columns.shape, jnp.float32),
            jax.ShapeDtypeStruct((steps,), jnp.float32),
        ),
        in_specs=[pl.BlockSpec(memory_space=pltpu.SMEM), vmem, vmem],
        out_specs=(pl.BlockSpec(memory_space=pl.ANY), pl.BlockSpec(memory_space=pltpu.SMEM)),
        scratch_shapes=[pltpu.SemaphoreType.DMA((2,))],
        name="place",
    )(plan, current, stat)


def solution(mesh):
    return jax.shard_map(
        local,
        mesh=mesh,
        in_specs=(P("blk", "rows"), P()),
        out_specs=(P("blk", "rows"), P()),
        check_vma=False,
    )
```
